32 devices in a mesh: gz: 8 (over z, x), rows: 4 (over y, core).
Axes of the slice: x: 2, y: 2, z: 4, core: 2. Of those that a mesh axis runs over, the one named last changes fastest.
Arguments:
- sections: bfloat16 [8, 1024, 4096], P('gz', 'rows'), may hold values from -4 to 4
- peaks: int32 [8, 2, 1, 4], P('gz'), may hold values from -16 to 16, as said below
Outputs:
- field: float32 [8, 2, 1024, 4096], P('gz', None, 'rows')
- pair_offsets: float32 [8, 2, 1, 4], P('gz')
- residual: bfloat16 [8, 1024, 4096], P('gz', 'rows')
The draws below stay inside these ranges and needn't reach their ends.
Inputs may be any that keep to these rules, and one draw needn't show every extreme that they name: `peaks`: in every draw the first section's first patch has row offset 16 and column offset -16.
All inputs are finite; a program needn't handle non-finite values.
Results may differ from the reference program's by a relative error of at most 0.001.
Values may be sent and summed in bfloat16 or wider, within the bound.
A program may use at most 64 MiB of HBM per device.

```python
import jax
import jax.numpy as jnp
import numpy as np
from jax import lax

W = 4096
PATCH = 1024
MAXOFF = 16
H = 1024
SECTIONS = 8
PGY = 1
PGX = 4


def joint_shifts(key):
    peaks = jax.random.randint(jax.random.fold_in(key, 11), (SECTIONS, 2, PGY, PGX), -MAXOFF, MAXOFF + 1)
    peaks = peaks.at[0, 0, 0, 0].set(MAXOFF).at[0, 1, 0, 0].set(-MAXOFF)
    fraction = jax.random.uniform(jax.random.fold_in(key, 12), (SECTIONS, 2, PGY, PGX), minval=-0.5, maxval=0.5)
    total = jnp.cumsum(peaks.astype(jnp.float32) + fraction, axis=0)
    return (peaks, total)


def draw_peaks(key, part):
    return joint_shifts(key)[0]


def draw_sections(key, part):
    _, total = joint_shifts(key)
    waves = 12
    wave_key = jax.random.fold_in(key, 13)
    length = jnp.exp(jax.random.uniform(jax.random.fold_in(wave_key, 1), (waves,), minval=jnp.log(12.0), maxval=jnp.log(64.0)))
    heading = jax.random.uniform(jax.random.fold_in(wave_key, 2), (waves,), minval=-3.14159, maxval=3.14159)
    phase = jax.random.uniform(jax.random.fold_in(wave_key, 3), (waves,), minval=-3.14159, maxval=3.14159)
    amplitude = 0.25 * jnp.ones((waves,), jnp.float32)
    noise_scale = 0.05
    freq_y = 6.2831853 / length * jnp.sin(heading)
    freq_x = 6.2831853 / length * jnp.cos(heading)
    row_index = jnp.arange(H)
    col_index = jnp.arange(W)
    patch_y = row_index // PATCH
    patch_x = col_index // PATCH
    noise_key = jax.random.fold_in(key, 14)

    def single(index):
        shift_y = total[index, 0][patch_y][:, patch_x]
        shift_x = total[index, 1][patch_y][:, patch_x]
        coord_y = row_index.astype(jnp.float32)[:, None] + shift_y
        coord_x = col_index.astype(jnp.float32)[None, :] + shift_x
        image = jnp.zeros((H, W), jnp.float32)
        for wave in range(waves):
            image = image + amplitude[wave] * jnp.cos(freq_y[wave] * coord_y + freq_x[wave] * coord_x + phase[wave])
        noise = jax.random.normal(jax.random.fold_in(noise_key, index), (H, W)) * noise_scale
        return jnp.clip(image + noise, -4.0, 4.0)
    return lax.map(single, jnp.arange(SECTIONS)).astype(jnp.bfloat16)


def setup_inputs(seed: int = 0) -> dict:
    streams_of = jax.random.split(jax.random.key(seed), 3)
    sections = draw_sections(jax.random.fold_in(streams_of[2], 71), 0)
    peaks = draw_peaks(jax.random.fold_in(streams_of[2], 71), 0)
    return dict(sections=sections, peaks=peaks)


LAMBDA = 0.002
RIDGE = 0.05


def invert_three(matrix):
    a, b, c = matrix[0, 0], matrix[0, 1], matrix[0, 2]
    d, e, f = matrix[1, 0], matrix[1, 1], matrix[1, 2]
    g, h, k = matrix[2, 0], matrix[2, 1], matrix[2, 2]
    cof = np.array([[e * k - f * h, c * h - b * k, b * f - c * e],
                    [f * g - d * k, a * k - c * g, c * d - a * f],
                    [d * h - e * g, b * g - a * h, a * e - b * d]])
    return cof / (a * (e * k - f * h) - b * (d * k - f * g) + c * (d * h - e * g))


def fit_table(pgy, pgx, patch, height, width):
    yy = ((np.arange(pgy) + 0.5) * patch - height / 2.0) / height
    xx = ((np.arange(pgx) + 0.5) * patch - width / 2.0) / width
    design = np.stack([np.repeat(yy, pgx), np.tile(xx, pgy), np.ones(pgy * pgx)], 1)
    ridge_matrix = np.array([[RIDGE, 0.0, 0.0], [0.0, RIDGE, 0.0], [0.0, 0.0, 0.0]])
    gram = design.T @ design + ridge_matrix
    return invert_three(gram) @ design.T


def spread(count, patch, nodes, start):
    pos = (start + jnp.arange(count).astype(jnp.float32) + 0.5) / patch - 0.5
    pos = jnp.clip(pos, 0.0, nodes - 1.0)
    return jnp.maximum(0.0, 1.0 - jnp.abs(pos[:, None] - jnp.arange(nodes).astype(jnp.float32)[None, :]))


def moments(current, window):
    centre = window[1:-1, 1:-1]
    grad_y = (window[2:, 1:-1] - window[:-2, 1:-1]) * 0.5
    grad_x = (window[1:-1, 2:] - window[1:-1, :-2]) * 0.5
    error = current - centre
    sums = jnp.stack([jnp.sum(grad_y * grad_y), jnp.sum(grad_y * grad_x), jnp.sum(grad_x * grad_x),
                      jnp.sum(grad_y * error), jnp.sum(grad_x * error)])
    return sums, error


def solve_pairs(sums, peak_grid):
    damping = LAMBDA * PATCH * PATCH
    first = sums[0] + damping
    cross = sums[1]
    second = sums[2] + damping
    determinant = first * second - cross * cross
    step_y = (second * sums[3] - cross * sums[4]) / determinant
    step_x = (first * sums[4] - cross * sums[3]) / determinant
    return peak_grid.astype(jnp.float32) + jnp.stack([step_y, step_x])


def transform(offsets, table, height, width):
    flat = offsets.reshape(2, -1)
    coef = jnp.dot(flat, table.T, precision=lax.Precision.HIGHEST)
    return jnp.eye(2, dtype=jnp.float32) + jnp.stack([coef[:, 0] / height, coef[:, 1] / width], axis=1)


def reference(sections, peaks):
    count, height, width = sections.shape
    pgy = height // PATCH
    pgx = width // PATCH
    margin = MAXOFF + 1
    table = jnp.asarray(fit_table(pgy, pgx, PATCH, height, width), jnp.float32)

    def pair(index):
        current = sections[index].astype(jnp.float32)
        before = jnp.where(index > 0, sections[jnp.maximum(index - 1, 0)].astype(jnp.float32), 0.0)
        padded = jnp.pad(before, margin)
        grid = peaks[index]
        rows_out = []
        errors_rows = []
        for i in range(pgy):
            cols_out = []
            errors_cols = []
            for j in range(pgx):
                start_y = (i * PATCH + margin - 1 + grid[0, i, j]).astype(jnp.int32)
                start_x = (j * PATCH + margin - 1 + grid[1, i, j]).astype(jnp.int32)
                window = lax.dynamic_slice(padded, (start_y, start_x), (PATCH + 2, PATCH + 2))
                piece = current[i * PATCH:(i + 1) * PATCH, j * PATCH:(j + 1) * PATCH]
                sums, error = moments(piece, window)
                cols_out.append(sums)
                errors_cols.append(error)
            rows_out.append(jnp.stack(cols_out, axis=1))
            errors_rows.append(jnp.concatenate(errors_cols, axis=1))
        sums = jnp.stack(rows_out, axis=1)
        image = jnp.concatenate(errors_rows, axis=0).astype(jnp.bfloat16)
        return solve_pairs(sums, grid), image

    offsets, residual = lax.map(pair, jnp.arange(count))

    def advance(carry, item):
        linear = transform(item, table, height, width)
        moved = jnp.dot(linear, carry, precision=lax.Precision.HIGHEST) + item.reshape(2, -1)
        return moved, moved

    _, cumulative = lax.scan(advance, jnp.zeros((2, pgy * pgx), jnp.float32), offsets)
    along_rows = spread(height, PATCH, pgy, 0)
    along_cols = spread(width, PATCH, pgx, 0)

    def dense(nodes):
        grid = nodes.reshape(2, pgy, pgx)
        wide = jnp.einsum('kij,cj->kic', grid, along_cols, precision=lax.Precision.HIGHEST)
        return jnp.einsum('ri,kic->krc', along_rows, wide, precision=lax.Precision.HIGHEST)

    field = lax.map(dense, cumulative)
    return field, offsets, residual
```

```python
import functools

import jax
import jax.numpy as jnp
import numpy as np
from jax import lax
from jax.experimental import pallas as pl
from jax.experimental.pallas import tpu as pltpu
from jax.sharding import PartitionSpec as P

PATCH = 1024
MAXOFF = 16
LAMBDA = 0.002
RIDGE = 0.05
EDGE = 32
SIDE = 128
BLOCK = 256
TILE = 64
MESH = pl.DeviceIdType.MESH


def invert_three(matrix):
    a, b, c = (matrix[0, 0], matrix[0, 1], matrix[0, 2])
    d, e, f = (matrix[1, 0], matrix[1, 1], matrix[1, 2])
    g, h, k = (matrix[2, 0], matrix[2, 1], matrix[2, 2])
    cof = np.array(
        [
            [e * k - f * h, c * h - b * k, b * f - c * e],
            [f * g - d * k, a * k - c * g, c * d - a * f],
            [d * h - e * g, b * g - a * h, a * e - b * d],
        ]
    )
    return cof / (a * (e * k - f * h) - b * (d * k - f * g) + c * (d * h - e * g))


def fit_table(pgy, pgx, patch, height, width):
    yy = ((np.arange(pgy) + 0.5) * patch - height / 2.0) / height
    xx = ((np.arange(pgx) + 0.5) * patch - width / 2.0) / width
    design = np.stack([np.repeat(yy, pgx), np.tile(xx, pgy), np.ones(pgy * pgx)], 1)
    ridge_matrix = np.array([[RIDGE, 0.0, 0.0], [0.0, RIDGE, 0.0], [0.0, 0.0, 0.0]])
    gram = design.T @ design + ridge_matrix
    return invert_three(gram) @ design.T


def register(G, R, pgy, pgx, table, peaks, sec, res_hbm, nodes, prev, cur, res, rmat, cmat, gmat, acc,
             sums, maps, cur_sem, res_sem, send_sem, recv_sem, rel_send, rel_recv,
             sum_send, sum_recv, map_send, map_recv):
    band, width = sec.shape[1], sec.shape[2]
    height = band * R
    blocks = width // BLOCK
    per_patch = PATCH // BLOCK
    g, r = lax.axis_index("gz"), lax.axis_index("rows")
    f32, bf16 = jnp.float32, jnp.bfloat16

    load = pltpu.make_async_copy(sec.at[0], cur, cur_sem)
    load.start()
    rows_all = band + 2 * EDGE
    prev[:, 0:SIDE] = jnp.zeros((rows_all, SIDE), bf16)
    prev[:, SIDE + width :] = jnp.zeros((rows_all, SIDE), bf16)

    @pl.when(r == 0)
    def _():
        prev[0:EDGE, :] = jnp.zeros((EDGE, width + 2 * SIDE), bf16)

    @pl.when(r == R - 1)
    def _():
        prev[EDGE + band :, :] = jnp.zeros((EDGE, width + 2 * SIDE), bf16)

    barrier = pltpu.get_barrier_semaphore()
    for d in range(1, R):
        pl.semaphore_signal(barrier, inc=1, device_id={"rows": lax.rem(r + d, R)}, device_id_type=MESH)
    for d in range(1, G):
        pl.semaphore_signal(barrier, inc=1, device_id={"gz": lax.rem(g + d, G)}, device_id_type=MESH)
    pl.semaphore_wait(barrier, R + G - 2)

    ahead = lax.rem(g + 1, G)

    def edge_copy(which):
        row = 0 if which == 0 else band - EDGE
        return pltpu.make_async_remote_copy(
            src_ref=sec.at[0, pl.ds(row, EDGE), :],
            dst_ref=prev.at[pl.ds(EDGE + row, EDGE), pl.ds(SIDE, width)],
            send_sem=send_sem.at[which], recv_sem=recv_sem.at[which],
            device_id={"gz": ahead}, device_id_type=MESH)

    def block_copy(c):
        col = pl.multiple_of(c * BLOCK, BLOCK)
        return pltpu.make_async_remote_copy(
            src_ref=sec.at[0, pl.ds(EDGE, band - 2 * EDGE), pl.ds(col, BLOCK)],
            dst_ref=prev.at[pl.ds(2 * EDGE, band - 2 * EDGE), pl.ds(SIDE + col, BLOCK)],
            send_sem=send_sem.at[2 + c], recv_sem=recv_sem.at[2 + c],
            device_id={"gz": ahead}, device_id_type=MESH)

    def relay_up():
        return pltpu.make_async_remote_copy(
            src_ref=prev.at[pl.ds(EDGE, EDGE), pl.ds(SIDE, width)],
            dst_ref=prev.at[pl.ds(EDGE + band, EDGE), pl.ds(SIDE, width)],
            send_sem=rel_send.at[0], recv_sem=rel_recv.at[0],
            device_id={"rows": lax.rem(r + R - 1, R)}, device_id_type=MESH)

    def relay_down():
        return pltpu.make_async_remote_copy(
            src_ref=prev.at[pl.ds(band, EDGE), pl.ds(SIDE, width)],
            dst_ref=prev.at[pl.ds(0, EDGE), pl.ds(SIDE, width)],
            send_sem=rel_send.at[1], recv_sem=rel_recv.at[1],
            device_id={"rows": lax.rem(r + 1, R)}, device_id_type=MESH)

    @pl.when(g < G - 1)
    def _():
        edge_copy(0).start()
        edge_copy(1).start()
        lax.fori_loop(0, blocks, lambda c, z: (block_copy(c).start(), z)[1], 0)

    @pl.when(g == 0)
    def _():
        def clear(t, z):
            prev[pl.ds(pl.multiple_of(t * EDGE, EDGE), EDGE), :] = jnp.zeros((EDGE, width + 2 * SIDE), bf16)
            return z

        lax.fori_loop(0, rows_all // EDGE, clear, 0)

    patch_row = r * band // PATCH
    rr = lax.broadcasted_iota(jnp.int32, (TILE, TILE + 2 * EDGE), 0)
    rk = lax.broadcasted_iota(jnp.int32, (TILE, TILE + 2 * EDGE), 1)
    ck = lax.broadcasted_iota(jnp.int32, (BLOCK + 2 * SIDE, BLOCK), 0)
    cn = lax.broadcasted_iota(jnp.int32, (BLOCK + 2 * SIDE, BLOCK), 1)
    rdiff = rk - rr - EDGE
    cdiff = ck - cn - SIDE
    for j in range(pgx):
        a = peaks[0, 0, patch_row, j]
        b = peaks[0, 1, patch_row, j]
        for n, step in enumerate((0, 1, -1)):
            rmat[j, n * TILE : (n + 1) * TILE, :] = jnp.where(rdiff == a + step, 1.0, 0.0).astype(bf16)
        cmat[j] = jnp.where(cdiff == b, 1.0, 0.0).astype(bf16)
        gmat[j] = jnp.where(cdiff == b + 1, 0.5, jnp.where(cdiff == b - 1, -0.5, 0.0)).astype(bf16)
    acc[...] = jnp.zeros_like(acc)
    load.wait()

    @pl.when(g > 0)
    def _():
        edge_copy(0).wait_recv()

        @pl.when(r > 0)
        def _():
            relay_up().start()

        edge_copy(1).wait_recv()

        @pl.when(r < R - 1)
        def _():
            relay_down().start()
            relay_up().wait_recv()

        @pl.when(r > 0)
        def _():
            relay_down().wait_recv()

        block_copy(0).wait_recv()

    tiles = band // TILE

    def fold(value):
        value = jnp.sum(value.reshape(value.shape[0] // 8, 8, BLOCK), axis=0)
        return sum(value[:, q : q + 128] for q in range(0, BLOCK, 128))

    def out_copy(c):
        col = pl.multiple_of(c * BLOCK, BLOCK)
        return pltpu.make_async_copy(res.at[:, pl.ds(col, BLOCK)], res_hbm.at[0, :, pl.ds(col, BLOCK)], res_sem.at[c])

    def body(c, z):
        @pl.when((g > 0) & (c + 1 < blocks))
        def _():
            block_copy(c + 1).wait_recv()

        j = c // per_patch
        col = pl.multiple_of(c * BLOCK, BLOCK)
        moved = []
        for t in range(tiles):
            window = prev[t * TILE : t * TILE + TILE + 2 * EDGE, pl.ds(col, BLOCK + 2 * SIDE)]
            moved.append(jnp.dot(rmat[j], window, preferred_element_type=f32).astype(bf16))
        parts = [jnp.concatenate([m[n * TILE : (n + 1) * TILE] for m in moved], axis=0) for n in range(3)]
        q = jnp.dot(parts[0], cmat[j], preferred_element_type=f32)
        lower = jnp.dot(parts[1], cmat[j], preferred_element_type=f32)
        upper = jnp.dot(parts[2], cmat[j], preferred_element_type=f32)
        gx = jnp.dot(parts[0], gmat[j], preferred_element_type=f32)
        gy = (lower - upper) * 0.5
        e = cur[:, pl.ds(col, BLOCK)].astype(f32) - q
        res[:, pl.ds(col, BLOCK)] = e.astype(bf16)
        out_copy(c).start()
        acc[j, 0] += fold(gy * gy)
        acc[j, 1] += fold(gy * gx)
        acc[j, 2] += fold(gx * gx)
        acc[j, 3] += fold(gy * e)
        acc[j, 4] += fold(gx * e)
        return z

    lax.fori_loop(0, blocks, body, 0)

    lane = lax.broadcasted_iota(jnp.int32, (8, 128), 1)
    row = lax.broadcasted_iota(jnp.int32, (8, 128), 0)
    mine = jnp.zeros((8, 128), f32)
    for j in range(pgx):
        for m in range(5):
            total = jnp.sum(jnp.sum(acc[j, m], axis=0, keepdims=True), axis=1, keepdims=True)
            mine = jnp.where((lane == patch_row * pgx + j) & (row == m), total, mine)
    sums[r] = mine

    def sum_copy(d, slot):
        return pltpu.make_async_remote_copy(
            src_ref=sums.at[slot], dst_ref=sums.at[slot], send_sem=sum_send.at[d], recv_sem=sum_recv.at[d],
            device_id={"rows": lax.rem(r + d, R)}, device_id_type=MESH)

    for d in range(1, R):
        sum_copy(d, r).start()
    peak_y = jnp.zeros((1, 128), f32)
    peak_x = jnp.zeros((1, 128), f32)
    for i in range(pgy):
        for j in range(pgx):
            here = lane[0:1] == i * pgx + j
            peak_y = jnp.where(here, peaks[0, 0, i, j].astype(f32), peak_y)
            peak_x = jnp.where(here, peaks[0, 1, i, j].astype(f32), peak_x)
    for d in range(1, R):
        sum_copy(d, lax.rem(r + R - d, R)).wait_recv()
    full = sums[0]
    for k in range(1, R):
        full = full + sums[k]

    damping = LAMBDA * PATCH * PATCH
    first = full[0:1] + damping
    cross = full[1:2]
    second = full[2:3] + damping
    det = first * second - cross * cross
    off_y = peak_y + (second * full[3:4] - cross * full[4:5]) / det
    off_x = peak_x + (first * full[4:5] - cross * full[3:4]) / det
    ty, tx = table[0:1], table[1:2]

    def lanes(value):
        return jnp.sum(value, axis=1, keepdims=True)

    pieces = [
        off_y,
        off_x,
        1.0 + lanes(off_y * ty) / height,
        lanes(off_y * tx) / width,
        lanes(off_x * ty) / height,
        1.0 + lanes(off_x * tx) / width,
    ]
    own = jnp.zeros((8, 128), f32)
    for k, piece in enumerate(pieces):
        own = jnp.where(row == k, jnp.broadcast_to(piece, (8, 128)), own)
    maps[g] = own

    def map_copy(d, slot):
        return pltpu.make_async_remote_copy(
            src_ref=maps.at[slot], dst_ref=maps.at[slot], send_sem=map_send.at[d], recv_sem=map_recv.at[d],
            device_id={"gz": lax.rem(g + d, G)}, device_id_type=MESH)

    for d in reversed(range(1, G)):
        @pl.when(g + d < G)
        def _():
            map_copy(d, g).start()

    for d in range(1, G):
        @pl.when(g - d >= 0)
        def _():
            map_copy(d, lax.rem(g + G - d, G)).wait_recv()

    def advance(s, u):
        uy, ux = u
        m = maps[s]
        return (m[2:3] * uy + m[3:4] * ux + m[0:1], m[4:5] * uy + m[5:6] * ux + m[1:2])

    zero = jnp.zeros((1, 128), f32)
    uy, ux = lax.fori_loop(0, g + 1, advance, (zero, zero))
    nodes[0:1] = uy
    nodes[1:2] = ux
    nodes[2:3] = off_y
    nodes[3:4] = off_x
    nodes[4:8] = jnp.zeros((4, 128), f32)

    lax.fori_loop(0, blocks, lambda c, z: (out_copy(c).wait(), z)[1], 0)

    @pl.when(g < G - 1)
    def _():
        edge_copy(0).wait_send()
        edge_copy(1).wait_send()
        lax.fori_loop(0, blocks, lambda c, z: (block_copy(c).wait_send(), z)[1], 0)

    @pl.when((g > 0) & (r > 0))
    def _():
        relay_up().wait_send()

    @pl.when((g > 0) & (r < R - 1))
    def _():
        relay_down().wait_send()

    for d in range(1, R):
        sum_copy(d, r).wait_send()
    for d in range(1, G):
        @pl.when(g + d < G)
        def _():
            map_copy(d, g).wait_send()


def spread_out(pgy, pgx, start_ref, nodes, res_in, field, offsets, res_out, buf, stage, in_sem, out_sem, field_sem):
    band, width = field.shape[2], field.shape[3]
    f32 = jnp.float32
    fetch = pltpu.make_async_copy(res_in, stage, in_sem)
    fetch.start()
    start = start_ref[0].astype(f32)
    cols = (lax.broadcasted_iota(jnp.int32, (1, width), 1).astype(f32) + 0.5) / PATCH - 0.5
    cols = jnp.clip(cols, 0.0, pgx - 1.0)
    weights = [jnp.maximum(0.0, 1.0 - jnp.abs(cols - j)) for j in range(pgx)]
    part = 64
    rows = lax.broadcasted_iota(jnp.int32, (part, 1), 0).astype(f32) + start
    put = pltpu.make_async_copy(stage, res_out, out_sem)
    copies = []
    for k in range(2):
        wide = []
        for i in range(pgy):
            line = jnp.zeros((1, width), f32)
            for j in range(pgx):
                p = i * pgx + j
                line = line + weights[j] * nodes[k : k + 1, p : p + 1]
            wide.append(line)
        for t in range(band // part):
            pos = jnp.clip((rows + (t * part + 0.5)) / PATCH - 0.5, 0.0, pgy - 1.0)
            block = jnp.zeros((part, width), f32)
            for i in range(pgy):
                block = block + jnp.maximum(0.0, 1.0 - jnp.abs(pos - i)) * wide[i]
            buf[k, t * part : (t + 1) * part, :] = block
            span = pl.ds(t * part, part)
            copy = pltpu.make_async_copy(buf.at[k, span, :], field.at[0, k, span, :], field_sem.at[len(copies)])
            copy.start()
            copies.append(copy)
        if k == 0:
            fetch.wait()
            put.start()
    offsets[...] = nodes[2:4, 0 : pgy * pgx]
    put.wait()
    for copy in copies:
        copy.wait()


def per_device(G, R, sections, peaks):
    band, width = sections.shape[1:]
    height = band * R
    pgy, pgx = height // PATCH, width // PATCH
    blocks = width // BLOCK
    f32, bf16 = jnp.float32, jnp.bfloat16
    table = np.zeros((8, 128), np.float32)
    table[:3, : pgy * pgx] = fit_table(pgy, pgx, PATCH, height, width)
    vmem = pl.BlockSpec(memory_space=pltpu.VMEM)
    smem = pl.BlockSpec(memory_space=pltpu.SMEM)
    anywhere = pl.BlockSpec(memory_space=pl.ANY)
    dma = pltpu.SemaphoreType.DMA
    residual, nodes = pl.pallas_call(
        functools.partial(register, G, R, pgy, pgx),
        name="register",
        out_shape=(jax.ShapeDtypeStruct((1, band, width), bf16), jax.ShapeDtypeStruct((8, 128), f32)),
        in_specs=[vmem, smem, anywhere],
        out_specs=(anywhere, vmem),
        scratch_shapes=[
            pltpu.VMEM((band + 2 * EDGE, width + 2 * SIDE), bf16),
            pltpu.VMEM((band, width), bf16),
            pltpu.VMEM((band, width), bf16),
            pltpu.VMEM((pgx, 3 * TILE, TILE + 2 * EDGE), bf16),
            pltpu.VMEM((pgx, BLOCK + 2 * SIDE, BLOCK), bf16),
            pltpu.VMEM((pgx, BLOCK + 2 * SIDE, BLOCK), bf16),
            pltpu.VMEM((pgx, 5, 8, 128), f32),
            pltpu.VMEM((R, 8, 128), f32),
            pltpu.VMEM((G, 8, 128), f32),
            dma, dma((blocks,)), dma((blocks + 2,)), dma((blocks + 2,)), dma((2,)), dma((2,)),
            dma((R,)), dma((R,)), dma((G,)), dma((G,)),
        ],
        compiler_params=pltpu.CompilerParams(collective_id=0, has_side_effects=True),
    )(jnp.asarray(table), peaks, sections)
    start = (lax.axis_index("rows") * band).astype(jnp.int32).reshape(1)
    field, offsets, residual = pl.pallas_call(
        functools.partial(spread_out, pgy, pgx),
        name="spread_out",
        out_shape=(
            jax.ShapeDtypeStruct((1, 2, band, width), f32),
            jax.ShapeDtypeStruct((2, pgy * pgx), f32),
            jax.ShapeDtypeStruct((1, band, width), bf16),
        ),
        in_specs=[smem, vmem, anywhere],
        out_specs=(anywhere, vmem, anywhere),
        scratch_shapes=[
            pltpu.VMEM((2, band, width), f32), pltpu.VMEM((1, band, width), bf16),
            dma, dma, dma((2 * (band // 64),)),
        ],
    )(start, nodes, residual)
    return field, offsets.reshape(1, 2, pgy, pgx), residual


def solution(mesh):
    return jax.shard_map(
        functools.partial(per_device, mesh.shape["gz"], mesh.shape["rows"]),
        mesh=mesh,
        in_specs=(P("gz", "rows", None), P("gz", None, None, None)),
        out_specs=(P("gz", None, "rows", None), P("gz", None, None, None), P("gz", "rows", None)),
        check_vma=False,
    )
```

```python
import functools

import jax
import jax.numpy as jnp
import numpy as np
from jax import lax
from jax.experimental import pallas as pl
from jax.experimental.pallas import tpu as pltpu
from jax.sharding import PartitionSpec as P

PATCH = 1024
MAXOFF = 16
LAMBDA = 0.002
RIDGE = 0.05
EDGE = 32
SIDE = 128
BLOCK = 256
TILE = 64
MESH = pl.DeviceIdType.MESH


def invert_three(matrix):
    a, b, c = (matrix[0, 0], matrix[0, 1], matrix[0, 2])
    d, e, f = (matrix[1, 0], matrix[1, 1], matrix[1, 2])
    g, h, k = (matrix[2, 0], matrix[2, 1], matrix[2, 2])
    cof = np.array(
        [
            [e * k - f * h, c * h - b * k, b * f - c * e],
            [f * g - d * k, a * k - c * g, c * d - a * f],
            [d * h - e * g, b * g - a * h, a * e - b * d],
        ]
    )
    return cof / (a * (e * k - f * h) - b * (d * k - f * g) + c * (d * h - e * g))


def fit_table(pgy, pgx, patch, height, width):
    yy = ((np.arange(pgy) + 0.5) * patch - height / 2.0) / height
    xx = ((np.arange(pgx) + 0.5) * patch - width / 2.0) / width
    design = np.stack([np.repeat(yy, pgx), np.tile(xx, pgy), np.ones(pgy * pgx)], 1)
    ridge_matrix = np.array([[RIDGE, 0.0, 0.0], [0.0, RIDGE, 0.0], [0.0, 0.0, 0.0]])
    gram = design.T @ design + ridge_matrix
    return invert_three(gram) @ design.T


def register(G, R, pgy, pgx, table, peaks_hbm, sec, res_hbm, nodes, prev, cur, res, rmat, cmat, gmat, acc,
             sums, maps, peaks, peak_sem, cur_sem, res_sem, send_sem, recv_sem, rel_send, rel_recv,
             sum_send, sum_recv, map_send, map_recv):
    band, width = sec.shape[1], sec.shape[2]
    height = band * R
    blocks = width // BLOCK
    per_patch = PATCH // BLOCK
    g, r = lax.axis_index("gz"), lax.axis_index("rows")
    f32, bf16 = jnp.float32, jnp.bfloat16

    barrier = pltpu.get_barrier_semaphore()
    for d in range(1, R):
        pl.semaphore_signal(barrier, inc=1, device_id={"rows": lax.rem(r + d, R)}, device_id_type=MESH)
    for d in range(1, G):
        pl.semaphore_signal(barrier, inc=1, device_id={"gz": lax.rem(g + d, G)}, device_id_type=MESH)
    peak_load = pltpu.make_async_copy(peaks_hbm, peaks, peak_sem)
    peak_load.start()
    load = pltpu.make_async_copy(sec.at[0], cur, cur_sem)
    load.start()
    rows_all = band + 2 * EDGE
    prev[:, 0:SIDE] = jnp.zeros((rows_all, SIDE), bf16)
    prev[:, SIDE + width :] = jnp.zeros((rows_all, SIDE), bf16)

    @pl.when(r == 0)
    def _():
        prev[0:EDGE, :] = jnp.zeros((EDGE, width + 2 * SIDE), bf16)

    @pl.when(r == R - 1)
    def _():
        prev[EDGE + band :, :] = jnp.zeros((EDGE, width + 2 * SIDE), bf16)

    pl.semaphore_wait(barrier, R + G - 2)

    ahead = lax.rem(g + 1, G)

    def edge_copy(which):
        row = 0 if which == 0 else band - EDGE
        return pltpu.make_async_remote_copy(
            src_ref=sec.at[0, pl.ds(row, EDGE), :],
            dst_ref=prev.at[pl.ds(EDGE + row, EDGE), pl.ds(SIDE, width)],
            send_sem=send_sem.at[which], recv_sem=recv_sem.at[which],
            device_id={"gz": ahead}, device_id_type=MESH)

    def span_copy(k, col, count):
        return pltpu.make_async_remote_copy(
            src_ref=sec.at[0, pl.ds(EDGE, band - 2 * EDGE), pl.ds(col, count)],
            dst_ref=prev.at[pl.ds(2 * EDGE, band - 2 * EDGE), pl.ds(SIDE + col, count)],
            send_sem=send_sem.at[2 + k], recv_sem=recv_sem.at[2 + k],
            device_id={"gz": ahead}, device_id_type=MESH)

    def head_copy():
        return span_copy(0, 0, BLOCK + SIDE)

    def middle_copy(k):
        return span_copy(k, pl.multiple_of(k * BLOCK + SIDE, SIDE), BLOCK)

    def tail_copy():
        return span_copy(blocks - 1, width - BLOCK + SIDE, BLOCK - SIDE)

    def relay_up():
        return pltpu.make_async_remote_copy(
            src_ref=prev.at[pl.ds(EDGE, EDGE), pl.ds(SIDE, width)],
            dst_ref=prev.at[pl.ds(EDGE + band, EDGE), pl.ds(SIDE, width)],
            send_sem=rel_send.at[0], recv_sem=rel_recv.at[0],
            device_id={"rows": lax.rem(r + R - 1, R)}, device_id_type=MESH)

    def relay_down():
        return pltpu.make_async_remote_copy(
            src_ref=prev.at[pl.ds(band, EDGE), pl.ds(SIDE, width)],
            dst_ref=prev.at[pl.ds(0, EDGE), pl.ds(SIDE, width)],
            send_sem=rel_send.at[1], recv_sem=rel_recv.at[1],
            device_id={"rows": lax.rem(r + 1, R)}, device_id_type=MESH)

    @pl.when(g < G - 1)
    def _():
        edge_copy(0).start()
        edge_copy(1).start()
        head_copy().start()
        lax.fori_loop(1, blocks - 1, lambda k, z: (middle_copy(k).start(), z)[1], 0)
        tail_copy().start()

    @pl.when(g == 0)
    def _():
        def clear(t, z):
            prev[pl.ds(pl.multiple_of(t * EDGE, EDGE), EDGE), :] = jnp.zeros((EDGE, width + 2 * SIDE), bf16)
            return z

        lax.fori_loop(0, rows_all // EDGE, clear, 0)

    patch_row = r * band // PATCH
    peak_load.wait()
    rr = lax.broadcasted_iota(jnp.int32, (TILE, TILE + 2 * EDGE), 0)
    rk = lax.broadcasted_iota(jnp.int32, (TILE, TILE + 2 * EDGE), 1)
    ck = lax.broadcasted_iota(jnp.int32, (BLOCK + 2 * SIDE, BLOCK), 0)
    cn = lax.broadcasted_iota(jnp.int32, (BLOCK + 2 * SIDE, BLOCK), 1)
    rdiff = rk - rr - EDGE
    cdiff = ck - cn - SIDE
    for j in range(pgx):
        a = peaks[0, 0, patch_row, j]
        b = peaks[0, 1, patch_row, j]
        for n, step in enumerate((0, 1, -1)):
            rmat[j, n * TILE : (n + 1) * TILE, :] = jnp.where(rdiff == a + step, 1.0, 0.0).astype(bf16)
        cmat[j] = jnp.where(cdiff == b, 1.0, 0.0).astype(bf16)
        gmat[j] = jnp.where(cdiff == b + 1, 0.5, jnp.where(cdiff == b - 1, -0.5, 0.0)).astype(bf16)
    acc[...] = jnp.zeros_like(acc)
    load.wait()

    @pl.when(g > 0)
    def _():
        edge_copy(0).wait_recv()

        @pl.when(r > 0)
        def _():
            relay_up().start()

        edge_copy(1).wait_recv()

        @pl.when(r < R - 1)
        def _():
            relay_down().start()
            relay_up().wait_recv()

        @pl.when(r > 0)
        def _():
            relay_down().wait_recv()

        head_copy().wait_recv()

    tiles = band // TILE

    def fold(value):
        value = jnp.sum(value.reshape(value.shape[0] // 8, 8, BLOCK), axis=0)
        return sum(value[:, q : q + 128] for q in range(0, BLOCK, 128))

    def out_copy(c):
        col = pl.multiple_of(c * BLOCK, BLOCK)
        return pltpu.make_async_copy(res.at[:, pl.ds(col, BLOCK)], res_hbm.at[0, :, pl.ds(col, BLOCK)], res_sem.at[c])

    def body(c, z):
        @pl.when((g > 0) & (c > 0) & (c < blocks - 1))
        def _():
            middle_copy(c).wait_recv()

        @pl.when((g > 0) & (c == blocks - 1))
        def _():
            tail_copy().wait_recv()

        j = c // per_patch
        col = pl.multiple_of(c * BLOCK, BLOCK)
        moved = []
        for t in range(tiles):
            window = prev[t * TILE : t * TILE + TILE + 2 * EDGE, pl.ds(col, BLOCK + 2 * SIDE)]
            moved.append(jnp.dot(rmat[j], window, preferred_element_type=f32).astype(bf16))
        parts = [jnp.concatenate([m[n * TILE : (n + 1) * TILE] for m in moved], axis=0) for n in range(3)]
        q = jnp.dot(parts[0], cmat[j], preferred_element_type=f32)
        lower = jnp.dot(parts[1], cmat[j], preferred_element_type=f32)
        upper = jnp.dot(parts[2], cmat[j], preferred_element_type=f32)
        gx = jnp.dot(parts[0], gmat[j], preferred_element_type=f32)
        gy = (lower - upper) * 0.5
        e = cur[:, pl.ds(col, BLOCK)].astype(f32) - q
        res[:, pl.ds(col, BLOCK)] = e.astype(bf16)
        out_copy(c).start()
        acc[j, 0] += fold(gy * gy)
        acc[j, 1] += fold(gy * gx)
        acc[j, 2] += fold(gx * gx)
        acc[j, 3] += fold(gy * e)
        acc[j, 4] += fold(gx * e)
        return z

    lax.fori_loop(0, blocks, body, 0)

    lane = lax.broadcasted_iota(jnp.int32, (8, 128), 1)
    row = lax.broadcasted_iota(jnp.int32, (8, 128), 0)
    mine = jnp.zeros((8, 128), f32)
    for j in range(pgx):
        for m in range(5):
            total = jnp.sum(jnp.sum(acc[j, m], axis=0, keepdims=True), axis=1, keepdims=True)
            mine = jnp.where((lane == patch_row * pgx + j) & (row == m), total, mine)
    sums[r] = mine

    def sum_copy(d, slot):
        return pltpu.make_async_remote_copy(
            src_ref=sums.at[slot], dst_ref=sums.at[slot], send_sem=sum_send.at[d], recv_sem=sum_recv.at[d],
            device_id={"rows": lax.rem(r + d, R)}, device_id_type=MESH)

    for d in range(1, R):
        sum_copy(d, r).start()
    peak_y = jnp.zeros((1, 128), f32)
    peak_x = jnp.zeros((1, 128), f32)
    for i in range(pgy):
        for j in range(pgx):
            here = lane[0:1] == i * pgx + j
            peak_y = jnp.where(here, peaks[0, 0, i, j].astype(f32), peak_y)
            peak_x = jnp.where(here, peaks[0, 1, i, j].astype(f32), peak_x)
    for d in range(1, R):
        sum_copy(d, lax.rem(r + R - d, R)).wait_recv()
    full = sums[0]
    for k in range(1, R):
        full = full + sums[k]

    damping = LAMBDA * PATCH * PATCH
    first = full[0:1] + damping
    cross = full[1:2]
    second = full[2:3] + damping
    det = first * second - cross * cross
    off_y = peak_y + (second * full[3:4] - cross * full[4:5]) / det
    off_x = peak_x + (first * full[4:5] - cross * full[3:4]) / det
    ty = jnp.zeros((1, 128), f32)
    tx = jnp.zeros((1, 128), f32)
    for p in range(pgy * pgx):
        ty = jnp.where(lane[0:1] == p, float(table[0, p]), ty)
        tx = jnp.where(lane[0:1] == p, float(table[1, p]), tx)

    def lanes(value):
        return jnp.sum(value, axis=1, keepdims=True)

    pieces = [
        off_y,
        off_x,
        1.0 + lanes(off_y * ty) / height,
        lanes(off_y * tx) / width,
        lanes(off_x * ty) / height,
        1.0 + lanes(off_x * tx) / width,
    ]
    own = jnp.zeros((8, 128), f32)
    for k, piece in enumerate(pieces):
        own = jnp.where(row == k, jnp.broadcast_to(piece, (8, 128)), own)
    maps[g] = own

    def map_copy(d, slot):
        return pltpu.make_async_remote_copy(
            src_ref=maps.at[slot], dst_ref=maps.at[slot], send_sem=map_send.at[d], recv_sem=map_recv.at[d],
            device_id={"gz": lax.rem(g + d, G)}, device_id_type=MESH)

    for d in reversed(range(1, G)):
        @pl.when(g + d < G)
        def _():
            map_copy(d, g).start()

    lax.fori_loop(0, blocks, lambda c, z: (out_copy(c).wait(), z)[1], 0)

    @pl.when(g < G - 1)
    def _():
        edge_copy(0).wait_send()
        edge_copy(1).wait_send()
        head_copy().wait_send()
        lax.fori_loop(1, blocks - 1, lambda k, z: (middle_copy(k).wait_send(), z)[1], 0)
        tail_copy().wait_send()

    @pl.when((g > 0) & (r > 0))
    def _():
        relay_up().wait_send()

    @pl.when((g > 0) & (r < R - 1))
    def _():
        relay_down().wait_send()

    for d in range(1, R):
        sum_copy(d, r).wait_send()
    for d in range(1, G):
        @pl.when(g - d >= 0)
        def _():
            map_copy(d, lax.rem(g + G - d, G)).wait_recv()

    def advance(s, u):
        uy, ux = u
        m = maps[s]
        return (m[2:3] * uy + m[3:4] * ux + m[0:1], m[4:5] * uy + m[5:6] * ux + m[1:2])

    zero = jnp.zeros((1, 128), f32)
    uy, ux = lax.fori_loop(0, g + 1, advance, (zero, zero))
    nodes[0:1] = uy
    nodes[1:2] = ux
    nodes[2:3] = off_y
    nodes[3:4] = off_x
    nodes[4:8] = jnp.zeros((4, 128), f32)

    for d in range(1, G):
        @pl.when(g + d < G)
        def _():
            map_copy(d, g).wait_send()


def spread_out(pgy, pgx, start_ref, nodes, res_in, field, offsets, res_out, buf, stage, in_sem, out_sem, field_sem):
    band, width = field.shape[2], field.shape[3]
    f32 = jnp.float32
    fetch = pltpu.make_async_copy(res_in, stage, in_sem)
    fetch.start()
    cols = (lax.broadcasted_iota(jnp.int32, (8, width), 1).astype(f32) + 0.5) / PATCH - 0.5
    cols = jnp.clip(cols, 0.0, pgx - 1.0)
    weights = [jnp.maximum(0.0, 1.0 - jnp.abs(cols - j)) for j in range(pgx)]
    part = 32
    put = pltpu.make_async_copy(stage, res_out, out_sem)
    copies = []
    for k in range(2):
        wide = []
        for i in range(pgy):
            line = jnp.zeros((8, width), f32)
            for j in range(pgx):
                p = i * pgx + j
                line = line + weights[j] * nodes[k : k + 1, p : p + 1]
            wide.append(line)
        for t in range(band // part):
            slot = 0 if pgy == 1 else t
            for q in range(0, part, 8) if pgy > 1 or t == 0 else ():
                if pgy == 1:
                    block = wide[0]
                else:
                    rows = lax.broadcasted_iota(jnp.int32, (8, 1), 0).astype(f32) + start_ref[0].astype(f32)
                    pos = jnp.clip((rows + (t * part + q + 0.5)) / PATCH - 0.5, 0.0, pgy - 1.0)
                    block = sum(jnp.maximum(0.0, 1.0 - jnp.abs(pos - i)) * wide[i] for i in range(pgy))
                buf[k, slot * part + q : slot * part + q + 8, :] = block
            copy = pltpu.make_async_copy(
                buf.at[k, pl.ds(slot * part, part), :], field.at[0, k, pl.ds(t * part, part), :],
                field_sem.at[len(copies)])
            copy.start()
            copies.append(copy)
        if k == 0:
            fetch.wait()
            put.start()
    offsets[...] = nodes[2:4, 0 : pgy * pgx]
    put.wait()
    for copy in copies:
        copy.wait()


def per_device(G, R, sections, peaks):
    band, width = sections.shape[1:]
    height = band * R
    pgy, pgx = height // PATCH, width // PATCH
    blocks = width // BLOCK
    f32, bf16 = jnp.float32, jnp.bfloat16
    table = fit_table(pgy, pgx, PATCH, height, width).astype(np.float32)
    vmem = pl.BlockSpec(memory_space=pltpu.VMEM)
    smem = pl.BlockSpec(memory_space=pltpu.SMEM)
    anywhere = pl.BlockSpec(memory_space=pl.ANY)
    dma = pltpu.SemaphoreType.DMA
    residual, nodes = pl.pallas_call(
        functools.partial(register, G, R, pgy, pgx, table),
        name="register",
        out_shape=(jax.ShapeDtypeStruct((1, band, width), bf16), jax.ShapeDtypeStruct((8, 128), f32)),
        in_specs=[anywhere, anywhere],
        out_specs=(anywhere, vmem),
        scratch_shapes=[
            pltpu.VMEM((band + 2 * EDGE, width + 2 * SIDE), bf16),
            pltpu.VMEM((band, width), bf16),
            pltpu.VMEM((band, width), bf16),
            pltpu.VMEM((pgx, 3 * TILE, TILE + 2 * EDGE), bf16),
            pltpu.VMEM((pgx, BLOCK + 2 * SIDE, BLOCK), bf16),
            pltpu.VMEM((pgx, BLOCK + 2 * SIDE, BLOCK), bf16),
            pltpu.VMEM((pgx, 5, 8, 128), f32),
            pltpu.VMEM((R, 8, 128), f32),
            pltpu.VMEM((G, 8, 128), f32),
            pltpu.SMEM((1, 2, pgy, pgx), jnp.int32),
            dma, dma, dma((blocks,)), dma((blocks + 2,)), dma((blocks + 2,)), dma((2,)), dma((2,)),
            dma((R,)), dma((R,)), dma((G,)), dma((G,)),
        ],
        compiler_params=pltpu.CompilerParams(collective_id=0, has_side_effects=True),
    )(peaks, sections)
    start = (lax.axis_index("rows") * band).astype(jnp.int32).reshape(1)
    field, offsets, residual = pl.pallas_call(
        functools.partial(spread_out, pgy, pgx),
        name="spread_out",
        out_shape=(
            jax.ShapeDtypeStruct((1, 2, band, width), f32),
            jax.ShapeDtypeStruct((2, pgy * pgx), f32),
            jax.ShapeDtypeStruct((1, band, width), bf16),
        ),
        in_specs=[smem, vmem, anywhere],
        out_specs=(anywhere, vmem, anywhere),
        scratch_shapes=[
            pltpu.VMEM((2, 32 if pgy == 1 else band, width), f32), pltpu.VMEM((1, band, width), bf16),
            dma, dma, dma((2 * (band // 32),)),
        ],
    )(start, nodes, residual)
    return field, offsets.reshape(1, 2, pgy, pgx), residual


def solution(mesh):
    return jax.shard_map(
        functools.partial(per_device, mesh.shape["gz"], mesh.shape["rows"]),
        mesh=mesh,
        in_specs=(P("gz", "rows", None), P("gz", None, None, None)),
        out_specs=(P("gz", None, "rows", None), P("gz", None, None, None), P("gz", "rows", None)),
        check_vma=False,
    )
```
